128 devices in a mesh: groups: 4 (over x, y), aux: 32 (over z, core).
Axes of the slice: x: 2, y: 2, z: 16, core: 2. Of those that a mesh axis runs over, the one named last changes fastest.
The devices are a block of a 8x8x16 slice.
Arguments:
- slabs: bfloat16 [16000, 23040], P(('groups', 'aux')), parts along dimension 0, may hold values from -2 to 2
- rdm: bfloat16 [3600, 900], P('groups'), parts along dimension 0, as said below
- orbital_energy: float32 [3072], P('groups'), parts along dimension 0, may hold values from 0.5 to 3
- pair_blocks: int32 [128, 2], P('groups'), parts along dimension 0, may hold values from 0 to 15, as said below
Outputs:
- pair_energy: float32 [6144, 48], P(('groups', 'aux')), parts along dimension 0
- window_energy: float32 [4], P('groups'), parts along dimension 0
The draws below stay inside these ranges and needn't reach their ends.
There are 4 independent parts, one for each index of `groups`. The reference program is written for one: setup_inputs(seed, part) draws one part's arguments, and reference() takes and returns one part's arrays. A program takes and returns all parts, laid end to end along the dimension named above; each array names one. Nothing has to cross between parts.
Inputs may be any that keep to these rules, and one draw needn't show every extreme that they name: `pair_blocks`: each row (p, q) has p <= q, and no two rows are equal. `rdm`: symmetric.
All inputs are finite; a program needn't handle non-finite values.
Results may differ from the reference program's by a relative error of at most 0.002.
Values may be sent and summed in bfloat16 or wider, within the bound.
No kernel may reach another device: no remote copies, remote signals or barrier semaphores. Data moves between devices by JAX's collectives and lax.ppermute only.
A program may use at most 128 MiB of HBM per device.

```python
import math
import jax
import jax.numpy as jnp
from jax import lax

NAUX = 4000
NACT = 30
VBLK = 48
NBLK = 16
NVIR = 768
N_AUX = 32


def draw_rdm(key, part):
    order = NACT * NACT
    first, second = jax.random.split(jax.random.fold_in(key, 11))
    base = jax.random.normal(first, (order, order), jnp.float32)
    spread = 0.5
    diagonal = jax.random.uniform(second, (order,), jnp.float32, 1.0, 2.0)
    symmetric = (base + base.T) * (spread / math.sqrt(2.0))
    return ((jnp.diag(diagonal) + symmetric) / order).astype(jnp.bfloat16)


def draw_pair_blocks(key, part):
    count = NBLK * (NBLK + 1) // 2
    chosen = jax.random.permutation(jax.random.fold_in(key, 23), count)[:N_AUX].astype(jnp.int32)
    rows = jnp.arange(NBLK, dtype=jnp.int32)
    starts = rows * NBLK - rows * (rows - 1) // 2
    first = jnp.sum((chosen[:, None] >= starts[None, 1:]).astype(jnp.int32), axis=1)
    begin = first * NBLK - first * (first - 1) // 2
    second = first + chosen - begin
    return jnp.stack([first, second], axis=1).astype(jnp.int32)


def levels(rng, shape, cuts, low, largest):
    loudness, own = 1.0, jax.random.fold_in(rng, 6)
    for position, shards_of in cuts:
        heights = jnp.exp(jax.random.uniform(jax.random.fold_in(own, position), (shards_of,), jnp.float32, low / len(cuts), largest / len(cuts)))
        loudness = loudness * jnp.repeat(heights, shape[position] // shards_of).reshape([-1 if axis == position else 1 for axis in range(len(shape))])
    return loudness


def centred(own_key, dims, width, reach, pieces=(), kind=jnp.bfloat16):
    entries = jax.random.normal(own_key, dims, jnp.float32) * width
    if len(pieces) > 0:
        entries = levels(own_key, dims, pieces, -0.22, 0.18) * entries
    return jnp.clip(entries, min=-reach, max=reach).astype(kind)


def setup_inputs(seed: int = 0, part: int = 0) -> dict:
    streams_of = jax.random.split(jax.random.key(seed), 5)
    part_splits = jax.random.split(jax.random.fold_in(streams_of[4], part), 5)
    slabs = centred(part_splits[0], (NAUX, NVIR * NACT), (1 / NAUX ** 0.25), 2.0, ((0, 32),))
    rdm = draw_rdm(jax.random.fold_in(jax.random.fold_in(streams_of[4], part), 71), part)
    orbital_energy = jnp.clip(jnp.exp(jax.random.uniform(part_splits[2], (NVIR,), jnp.float32, math.log(0.5), math.log(3.0))), 0.5, 3.0)
    pair_blocks = draw_pair_blocks(jax.random.fold_in(jax.random.fold_in(streams_of[4], part), 71), part)
    return dict(slabs=slabs, rdm=rdm, orbital_energy=orbital_energy, pair_blocks=pair_blocks)


def reference(slabs, rdm, orbital_energy, pair_blocks):
    blocked = slabs.reshape(NAUX, NBLK, VBLK * NACT)
    energy_table = orbital_energy.reshape(NBLK, VBLK)

    def one_pair(blocks):
        row_part = blocked[:, blocks[0]]
        col_part = blocked[:, blocks[1]]
        integrals = lax.dot_general(row_part, col_part, (((0,), (0,)), ((), ())), preferred_element_type=jnp.float32).astype(jnp.bfloat16)
        reordered = integrals.reshape(VBLK, NACT, VBLK, NACT).transpose(0, 2, 1, 3).reshape(VBLK * VBLK, NACT * NACT)
        contracted = jnp.dot(reordered, rdm, preferred_element_type=jnp.float32)
        paired = jnp.sum(contracted * reordered.astype(jnp.float32), axis=1).reshape(VBLK, VBLK)
        energy = -paired / (energy_table[blocks[0]][:, None] + energy_table[blocks[1]][None, :])
        weight = jnp.where(blocks[0] == blocks[1], jnp.float32(1.0), jnp.float32(2.0))
        return energy, weight * jnp.sum(energy)

    energies, totals = lax.map(one_pair, pair_blocks)
    mean_energy = jnp.sum(totals) / (VBLK * VBLK * N_AUX)
    return energies.reshape(N_AUX * VBLK, VBLK), mean_energy.reshape(1)
```

```python
import numpy as np
import jax
import jax.numpy as jnp
from jax import lax
from jax.experimental import pallas as pl
from jax.experimental.pallas import tpu as pltpu
from jax.sharding import PartitionSpec as P


NACT = 30
VBLK = 48
NBLK = 16
WIDTH = VBLK * NACT
LANES = 128
CORES = 2
CHIPS = 16
BELOW = 2
ABOVE = 3
LONGEST = 10
JOBS = 2
TPAD = 32
PACKED = NACT * TPAD
STEPS = 256
OFFSETS = range(-ABOVE, BELOW + 1)


def swap_plan():
    draw = np.random.default_rng(7)
    first = draw.integers(0, NBLK, STEPS)
    second = (first + draw.integers(1, NBLK, STEPS)) % NBLK
    heat = 0.7 * (0.2 / 0.7) ** (np.arange(STEPS) / STEPS)
    heat[:24] = 4.0
    return (
        np.stack([first, second], axis=1).astype(np.int32).reshape(-1),
        (1.0 / heat).astype(np.float32),
    )


def ring_mask(reach):
    return sum(1 << d for d in range(NBLK) if min(d, NBLK - d) in reach)


def plan_kernel(me, pairs, swaps, coolness, table, words, links, home, load):
    far_base = ring_mask(range(BELOW + ABOVE + 1, NBLK))
    edge_base = ring_mask([BELOW + ABOVE])
    near_edge_base = ring_mask([BELOW + ABOVE - 1])
    shape = (8, 128)

    def turned(base, z):
        return ((base << z) | (base >> (NBLK - z))) & 0xFFFF

    def count(x):
        return lax.population_count(x)

    def clear(z, c):
        links[z] = 0
        load[z] = 0
        return c

    lax.fori_loop(0, NBLK, clear, 0)
    n_pairs = pairs.shape[0] // 2

    def link(d, c):
        p = pairs[2 * d]
        q = pairs[2 * d + 1]
        differ = jnp.where(p == q, 0, 1)
        links[p] = links[p] | (differ << q)
        links[q] = links[q] | (differ << p)
        return c

    lax.fori_loop(0, n_pairs, link, 0)
    cost = jnp.zeros(shape, jnp.int32)
    for z in range(NBLK):
        word = jnp.broadcast_to(links[z] | (z << 16), shape).astype(jnp.int32)
        words[z] = word
        cost = cost + count(word & turned(far_base, z))
    cost = cost // 2
    lane = lax.broadcasted_iota(jnp.int32, shape, 0) * 128 + lax.broadcasted_iota(jnp.int32, shape, 1)
    noise = (lane * 747796405 + 12345) * 1103515245 + 12345

    def step(i, carry):
        cost, noise = carry
        x = swaps[2 * i]
        y = swaps[2 * i + 1]
        wx = words[x]
        wy = words[y]

        def crossed(w):
            t = ((w >> x) ^ (w >> y)) & 1
            return w ^ ((t << x) | (t << y))

        far_x = turned(jnp.int32(far_base), x)
        far_y = turned(jnp.int32(far_base), y)
        change = (
            count(crossed(wy) & far_x)
            + count(crossed(wx) & far_y)
            - count(wx & far_x)
            - count(wy & far_y)
        )
        noise = noise * 1664525 + 1013904223
        chance = ((noise >> 8) & 0xFFFF).astype(jnp.float32) * (1.0 / 65536.0)
        bound = jnp.exp(change.astype(jnp.float32) * (-coolness[i]))
        take = ((change <= 0) | (chance < bound)) & (cost > 0)
        take_bit = take.astype(jnp.int32)
        for z in range(NBLK):
            w = words[z]
            t = ((w >> x) ^ (w >> y)) & take_bit
            words[z] = w ^ ((t << x) | (t << y))
        wx = words[x]
        wy = words[y]
        words[x] = jnp.where(take, wy, wx)
        words[y] = jnp.where(take, wx, wy)
        return cost + change * take_bit, noise

    cost, noise = lax.fori_loop(0, STEPS, step, (cost, noise))
    tight = jnp.zeros(shape, jnp.int32)
    for z in range(NBLK):
        w = words[z]
        tight = tight + 2 * count(w & turned(edge_base, z)) + count(w & turned(near_edge_base, z))
    score = jnp.minimum(cost * 512 + tight, 16000) * 1024 + lane
    best = jnp.min(score.astype(jnp.float32))
    chosen = score.astype(jnp.float32) == best
    for z in range(NBLK):
        w = jnp.sum(jnp.where(chosen, words[z].astype(jnp.float32), 0.0)).astype(jnp.int32)
        home[(w >> 16) & 15] = z

    def span(d):
        x = home[pairs[2 * d]]
        y = home[pairs[2 * d + 1]]
        ahead = (y - x) & (NBLK - 1)
        forward = ahead <= NBLK // 2
        gap = jnp.where(forward, ahead, NBLK - ahead)
        low = jnp.where(forward, y, x) - BELOW
        return gap, low

    def rank(r, unfit):
        def place(d, unfit):
            gap, low = span(d)

            def choose(c, best_chip):
                chip = (low + c) & (NBLK - 1)
                better = load[chip] < load[best_chip]
                return jnp.where(better, chip, best_chip)

            now = gap == BELOW + ABOVE - r
            spot = lax.fori_loop(1, jnp.where(now, r + 1, 1), choose, low & (NBLK - 1))

            @pl.when(now)
            def _():
                turn = load[spot]
                load[spot] = turn + 1
                table[24 + d] = jnp.minimum((spot * CORES + turn % CORES) * JOBS + turn // CORES, n_pairs * JOBS - 1)
                here = (spot == me[0] // CORES) & (turn < CORES * JOBS)

                @pl.when(turn >= CORES)
                def _():
                    table[17] = 1

                @pl.when(here)
                def _():
                    whose = jnp.where(turn % CORES == me[0] % CORES, MINE, OTHERS)
                    slot = whose + 3 * (turn // CORES)
                    table[slot] = 1
                    table[slot + 1] = ((home[pairs[2 * d]] - spot + 8) & 15) - 8
                    table[slot + 2] = ((home[pairs[2 * d + 1]] - spot + 8) & 15) - 8

            full = now & (load[spot] > CORES * JOBS)
            return unfit + jnp.where(full, 1, 0)

        return lax.fori_loop(0, n_pairs, place, unfit)

    for j in range(8 * JOBS):
        table[MINE + j] = 0
    table[17] = 0

    def missed(d, c):
        table[24 + d] = 0
        return c + jnp.where(span(d)[0] > BELOW + ABOVE, 1, 0)

    unfit = lax.fori_loop(0, n_pairs, missed, 0)
    unfit = lax.fori_loop(0, BELOW + ABOVE + 1, rank, unfit)
    table[0] = jnp.where(unfit == 0, 1, 0)
    for z in range(NBLK):
        table[1 + z] = home[z]


def make_plan(me, pair_blocks):
    swaps, coolness = swap_plan()
    smem = pl.BlockSpec(memory_space=pltpu.SMEM)
    return pl.pallas_call(
        plan_kernel,
        out_shape=jax.ShapeDtypeStruct((96,), jnp.int32),
        in_specs=[smem] * 4,
        out_specs=smem,
        scratch_shapes=[
            pltpu.VMEM((NBLK, 8, 128), jnp.int32),
            pltpu.SMEM((NBLK,), jnp.int32),
            pltpu.SMEM((NBLK,), jnp.int32),
            pltpu.SMEM((NBLK,), jnp.int32),
        ],
        name="plan",
    )(me, pair_blocks.reshape(-1), jnp.asarray(swaps), jnp.asarray(coolness))


PER_STEP = 4


def pack_kernel(me, table, slab, *rest):
    outs = rest[: 2 * LONGEST]
    turned, packed, sems = rest[2 * LONGEST :]
    g = pl.program_id(0)
    chip = me[0] // CORES
    rows = slab.shape[0]

    def copies(b):
        o = ((table[1 + b] - chip + 8) & 15) - 8
        for reach in range(1, LONGEST + 1):
            yield o == reach - ABOVE, pltpu.make_async_copy(packed.at[b], outs[reach - 1], sems.at[reach - 1])
            yield o == BELOW - reach, pltpu.make_async_copy(
                packed.at[b], outs[LONGEST + reach - 1], sems.at[LONGEST + reach - 1]
            )

    for i in range(PER_STEP):
        b = g * PER_STEP + i
        part = slab[:, i * WIDTH : (i + 1) * WIDTH].astype(jnp.float32)
        part = jnp.concatenate([part, jnp.zeros((LANES - rows, WIDTH), jnp.float32)], axis=0)
        turned[...] = part.T
        for t in range(NACT):
            packed[b, t * VBLK : (t + 1) * VBLK, :] = turned[pl.ds(t, VBLK, stride=NACT), :].astype(jnp.bfloat16)
        for when, copy in copies(b):

            @pl.when(when)
            def _(copy=copy):
                copy.start()

    @pl.when(g == NBLK // PER_STEP - 1)
    def _():
        for n in range(2 * LONGEST):
            pltpu.make_async_copy(packed.at[0], outs[n], sems.at[n]).wait()


def pack(me, table, slabs):
    rows = slabs.shape[0]
    smem = pl.BlockSpec(memory_space=pltpu.SMEM)
    return pl.pallas_call(
        pack_kernel,
        grid=(NBLK // PER_STEP,),
        in_specs=[smem, smem, pl.BlockSpec((rows, PER_STEP * WIDTH), lambda g: (0, g))],
        out_specs=[pl.BlockSpec(memory_space=pl.ANY)] * (2 * LONGEST),
        out_shape=[jax.ShapeDtypeStruct((WIDTH, LANES), jnp.bfloat16)] * (2 * LONGEST),
        scratch_shapes=[
            pltpu.VMEM((WIDTH, LANES), jnp.float32),
            pltpu.VMEM((NBLK, WIDTH, LANES), jnp.bfloat16),
            pltpu.SemaphoreType.DMA((2 * LONGEST,)),
        ],
        compiler_params=pltpu.CompilerParams(vmem_limit_bytes=40 * 1024 * 1024),
        name="pack",
    )(me, table, slabs)


ROW_TILE = 480
TILES = -(-WIDTH // LANES)
COL_TILES = ((0, 512), (512, 512), (1024, 416))
GROUP = 8
HBM = pltpu.MemorySpace.HBM
MINE = 64
OTHERS = 72


def unflatten(refs, sources):
    refs = list(refs)
    return [{d: refs.pop(0) for d in OFFSETS} for _ in sources]


def flatten(pieces, sources):
    return [pieces[s][d] for s in sources for d in OFFSETS]


def select_kernel(table, *rest, sources, job):
    count = len(sources) * len(OFFSETS)
    pieces = unflatten(rest[:count], sources)
    out, held, sems, out_sem = rest[count:]

    @pl.when(table[OTHERS + 3 * job] == 1)
    def _():
        for side in range(2):
            wanted = table[OTHERS + 3 * job + 1 + side]
            for n in range(len(sources)):
                for d, piece in pieces[n].items():

                    @pl.when(wanted == d)
                    def _(piece=piece, n=n, side=side):
                        pltpu.make_async_copy(piece, held.at[side, n], sems.at[side, n]).start()

        for side in range(2):
            for n in range(len(sources)):
                pltpu.make_async_copy(next(iter(pieces[n].values())), held.at[side, n], sems.at[side, n]).wait()
                pltpu.make_async_copy(held.at[side, n], out.at[side, n], out_sem.at[side, n]).start()
        for side in range(2):
            for n in range(len(sources)):
                pltpu.make_async_copy(held.at[side, n], out.at[side, n], out_sem.at[side, n]).wait()


def select(table, pieces, sources, job):
    flat = flatten(pieces, sources)
    n = len(sources)
    return pl.pallas_call(
        lambda *refs: select_kernel(*refs, sources=sources, job=job),
        in_specs=[pl.BlockSpec(memory_space=pltpu.SMEM)] + [pl.BlockSpec(memory_space=HBM)] * len(flat),
        out_specs=pl.BlockSpec(memory_space=HBM),
        out_shape=jax.ShapeDtypeStruct((2, n, WIDTH, LANES), jnp.bfloat16),
        scratch_shapes=[
            pltpu.VMEM((2, n, WIDTH, LANES), jnp.bfloat16),
            pltpu.SemaphoreType.DMA((2, n)),
            pltpu.SemaphoreType.DMA((2, n)),
        ],
        name="select",
    )(table, *flat)


def multiply(table, job, pieces, other, bufs, sems, acc, fresh):
    def lanes(n, who):
        return pl.ds((n * CORES + who) * LANES, LANES)

    for side, buf in enumerate(bufs):
        wanted = table[MINE + 3 * job + 1 + side]
        for n in range(len(pieces)):
            pltpu.make_async_copy(other.at[side, n], buf.at[:, lanes(n, 1)], sems.at[side, n, 1]).start()
            for d, piece in pieces[n].items():

                @pl.when(wanted == d)
                def _(piece=piece, n=n, side=side, buf=buf):
                    pltpu.make_async_copy(piece, buf.at[:, lanes(n, 0)], sems.at[side, n, 0]).start()

    for side, buf in enumerate(bufs):
        for n in range(len(pieces)):
            for who in range(CORES):
                pltpu.make_async_copy(other.at[side, n], buf.at[:, lanes(n, who)], sems.at[side, n, who]).wait()
    col_buf, row_buf = bufs

    def rows(m, c):
        here = pl.ds(pl.multiple_of(m * ROW_TILE, ROW_TILE), ROW_TILE)
        left = row_buf[here, :]
        for start, size in COL_TILES:
            part = lax.dot_general(
                left, col_buf[start : start + size, :], (((1,), (1,)), ((), ())), preferred_element_type=jnp.float32
            )
            for at in range(0, size, LANES):
                wide = min(LANES, size - at)
                tile = acc.at[(start + at) // LANES, here, pl.ds(0, wide)]
                if fresh:
                    tile[...] = part[:, at : at + wide]
                else:
                    tile[...] += part[:, at : at + wide]
        return c

    lax.fori_loop(0, WIDTH // ROW_TILE, rows, 0)


def early_kernel(table, other, *rest, sources, job, fresh):
    before = None
    if not fresh:
        before, *rest = rest
    count = len(sources) * len(OFFSETS)
    pieces = unflatten(rest[:count], sources)
    out, col_buf, row_buf, acc, sems, sem = rest[count:]

    @pl.when(table[MINE + 3 * job] == 1)
    def _():
        if not fresh:
            copy = pltpu.make_async_copy(before, acc, sem)
            copy.start()
            copy.wait()
        multiply(table, job, pieces, other, (col_buf, row_buf), sems, acc, fresh)
        copy = pltpu.make_async_copy(acc, out, sem)
        copy.start()
        copy.wait()


def density_kernel(rdm, out, wide, lifted):
    out[...] = jnp.zeros(out.shape, out.dtype)
    lifted[...] = jnp.zeros(lifted.shape, jnp.float32)
    wide[...] = rdm[...].astype(jnp.float32)
    for v in range(NACT):
        lifted[:, v * TPAD : v * TPAD + NACT] = wide[:, v * NACT : (v + 1) * NACT]
    for t in range(NACT):
        out[t * TPAD : t * TPAD + NACT, :] = lifted[t * NACT : (t + 1) * NACT, :].astype(jnp.bfloat16)


def spread_density(rdm):
    order = NACT * NACT
    return pl.pallas_call(
        density_kernel,
        out_shape=jax.ShapeDtypeStruct((PACKED, PACKED), jnp.bfloat16),
        scratch_shapes=[pltpu.VMEM((order, order), jnp.float32), pltpu.VMEM((order, PACKED), jnp.float32)],
        name="density",
    )(rdm)


def finish_kernel(table, other, before, density, *rest, sources, job):
    count = len(sources) * len(OFFSETS)
    pieces = unflatten(rest[:count], sources)
    out, col_buf, row_buf, acc, spread, sems, sem = rest[count:]

    @pl.when(table[MINE + 3 * job] == 0)
    def _():
        out[...] = jnp.zeros(out.shape, out.dtype)

    @pl.when(table[MINE + 3 * job] == 1)
    def _():
        copy = pltpu.make_async_copy(before, acc.at[:, pl.ds(0, WIDTH), :], sem)
        copy.start()
        acc[:, WIDTH:, :] = jnp.zeros((TILES, acc.shape[1] - WIDTH, LANES), jnp.float32)
        copy.wait()
        multiply(table, job, pieces, other, (col_buf, row_buf), sems, acc, False)

        def group(g, carry):
            for i in range(GROUP):
                here = pl.ds(g * GROUP + i, TPAD, stride=VBLK)
                rows = jnp.concatenate([acc[c, here, :] for c in range(TILES)], axis=1).astype(jnp.bfloat16)
                for t in range(NACT):
                    spread[t * TPAD : (t + 1) * TPAD, i * VBLK : (i + 1) * VBLK] = rows[:, t * VBLK : (t + 1) * VBLK]
            x = spread[...]
            y = jnp.dot(density[...], x, preferred_element_type=jnp.float32)
            out[pl.ds(g, 1), :] = jnp.sum(y * x.astype(jnp.float32), axis=0, keepdims=True)
            return carry

        lax.fori_loop(0, VBLK // GROUP, group, 0)


def product_scratch(sources, rows):
    depth = len(sources) * CORES * LANES
    return [
        pltpu.VMEM((WIDTH, depth), jnp.bfloat16),
        pltpu.VMEM((WIDTH, depth), jnp.bfloat16),
        pltpu.VMEM((TILES, rows, LANES), jnp.float32),
    ]


ROOM = pltpu.CompilerParams(vmem_limit_bytes=48 * 1024 * 1024)


def early(table, other, before, pieces, sources, job):
    flat = flatten(pieces, sources)
    fresh = before is None
    held = [] if fresh else [before]
    in_hbm = pl.BlockSpec(memory_space=HBM)
    return pl.pallas_call(
        lambda *refs: early_kernel(*refs, sources=sources, job=job, fresh=fresh),
        in_specs=[pl.BlockSpec(memory_space=pltpu.SMEM)] + [in_hbm] * (1 + len(held) + len(flat)),
        out_specs=in_hbm,
        out_shape=jax.ShapeDtypeStruct((TILES, WIDTH, LANES), jnp.float32),
        scratch_shapes=product_scratch(sources, WIDTH)
        + [pltpu.SemaphoreType.DMA((2, len(sources), CORES)), pltpu.SemaphoreType.DMA],
        compiler_params=ROOM,
        name="early",
    )(table, other, *held, *flat)


def finish(table, other, before, density, pieces, sources, job):
    flat = flatten(pieces, sources)
    in_hbm = pl.BlockSpec(memory_space=HBM)
    return pl.pallas_call(
        lambda *refs: finish_kernel(*refs, sources=sources, job=job),
        in_specs=[pl.BlockSpec(memory_space=pltpu.SMEM), in_hbm, in_hbm, pl.BlockSpec(memory_space=pltpu.VMEM)]
        + [in_hbm] * len(flat),
        out_specs=pl.BlockSpec(memory_space=pltpu.VMEM),
        out_shape=jax.ShapeDtypeStruct((VBLK // GROUP, GROUP * VBLK), jnp.float32),
        scratch_shapes=product_scratch(sources, VBLK * TPAD)
        + [
            pltpu.VMEM((PACKED, GROUP * VBLK), jnp.bfloat16),
            pltpu.SemaphoreType.DMA((2, len(sources), CORES)),
            pltpu.SemaphoreType.DMA,
        ],
        compiler_params=ROOM,
        name="finish",
    )(table, other, before, density, *flat)


def ring_shift(hops):
    n = lax.axis_size("aux")
    return [(i, (i + hops * CORES) % n) for i in range(n)]


def to_other_core(x):
    n = lax.axis_size("aux")
    return lax.ppermute(x, "aux", [(i, i ^ 1) for i in range(n)])


def energies_of(paired, orbital_energy, pair_blocks):
    table = orbital_energy.reshape(NBLK, VBLK)
    rows = table[pair_blocks[:, 0]]
    cols = table[pair_blocks[:, 1]]
    energy = -paired / (rows[:, :, None] + cols[:, None, :])
    weight = jnp.where(pair_blocks[:, 0] == pair_blocks[:, 1], jnp.float32(1.0), jnp.float32(2.0))
    total = jnp.sum(weight * jnp.sum(energy, axis=(1, 2)))
    mine = lax.dynamic_index_in_dim(energy, lax.axis_index("aux"), 0, keepdims=False)
    mean_energy = total / (VBLK * VBLK * lax.axis_size("aux"))
    return mine, mean_energy.reshape(1)


def sources_within(low, high):
    return [s for s in range(-CHIPS // 2, CHIPS // 2) if low <= abs(s) <= high]


NEAREST = sources_within(0, 3)
NEAR = sources_within(4, 5)
FAR = sources_within(6, CHIPS)


def planned(table, me, slabs, rdm, orbital_energy, pair_blocks):
    sent = pack(me, table, slabs)
    pieces = {s: {} for s in range(-CHIPS // 2, CHIPS // 2)}

    def keep(source, offset, value):
        if -ABOVE <= offset <= BELOW:
            pieces[(source + CHIPS // 2) % CHIPS - CHIPS // 2][offset] = value

    right = {reach: sent[reach - 1] for reach in range(1, LONGEST + 1)}
    left = {reach: sent[LONGEST + reach - 1] for reach in range(1, LONGEST + 1)}
    for offset in OFFSETS:
        keep(0, offset, right[offset + ABOVE] if offset > -ABOVE else left[BELOW + ABOVE])
    sums = None
    density = None

    def exchange(sources, job):
        chosen = select(table, pieces, sources, job)
        return to_other_core(chosen)

    for hop in range(1, LONGEST + 1):
        for reach in range(LONGEST, hop - 1, -1):
            right[reach] = lax.ppermute(right[reach], "aux", ring_shift(1))
            left[reach] = lax.ppermute(left[reach], "aux", ring_shift(-1))
            keep(-hop, reach - ABOVE - hop, right[reach])
            keep(hop, BELOW - reach + hop, left[reach])
        if hop == 1:
            density = spread_density(rdm)
        if hop == 3:
            other = exchange(NEAREST, 0)
            sums = early(table, other, None, pieces, NEAREST, 0)
        if hop == 5:
            other = exchange(NEAR, 0)
            sums = early(table, other, sums, pieces, NEAR, 0)
    other = exchange(FAR, 0)
    paired = finish(table, other, sums, density, pieces, FAR, 0)

    def second_job(pieces):
        other = exchange(NEAREST, 1)
        sums = early(table, other, None, pieces, NEAREST, 1)
        other = exchange(NEAR, 1)
        sums = early(table, other, sums, pieces, NEAR, 1)
        other = exchange(FAR, 1)
        return finish(table, other, sums, density, pieces, FAR, 1)

    extra = lax.cond(table[17] == 1, second_job, lambda pieces: jnp.zeros_like(paired), pieces)
    everyone = lax.all_gather(jnp.stack([paired, extra]), "aux").reshape(-1, VBLK, VBLK)
    paired = everyone[lax.dynamic_slice_in_dim(table, 24, pair_blocks.shape[0])].transpose(0, 2, 1)
    return energies_of(paired, orbital_energy, pair_blocks)


def unplanned(table, me, slabs, rdm, orbital_energy, pair_blocks):
    local_rows = slabs.shape[0]
    blocked = slabs.reshape(local_rows, NBLK, WIDTH)
    sides = []
    for side in range(2):
        outgoing = jnp.take(blocked, pair_blocks[:, side], axis=1)
        arrived = lax.all_to_all(outgoing, "aux", split_axis=1, concat_axis=0, tiled=True)
        sides.append(arrived.reshape(-1, WIDTH))
    products = lax.dot_general(sides[0], sides[1], (((0,), (0,)), ((), ())), preferred_element_type=jnp.float32)
    reordered = (
        products.astype(jnp.bfloat16)
        .reshape(VBLK, NACT, VBLK, NACT)
        .transpose(0, 2, 1, 3)
        .reshape(VBLK * VBLK, NACT * NACT)
    )
    contracted = jnp.dot(reordered, rdm, preferred_element_type=jnp.float32)
    paired = jnp.sum(contracted * reordered.astype(jnp.float32), axis=1).reshape(VBLK, VBLK)
    return energies_of(lax.all_gather(paired, "aux"), orbital_energy, pair_blocks)


def per_device(slabs, rdm, orbital_energy, pair_blocks):
    me = lax.axis_index("aux").reshape(1).astype(jnp.int32)
    table = make_plan(me, pair_blocks)
    return lax.cond(table[0] == 1, planned, unplanned, table, me, slabs, rdm, orbital_energy, pair_blocks)


def solution(mesh):
    return jax.shard_map(
        per_device,
        mesh=mesh,
        in_specs=(P(("groups", "aux"), None), P("groups", None), P("groups"), P("groups", None)),
        out_specs=(P(("groups", "aux"), None), P("groups")),
        check_vma=False,
    )
```

```python
import numpy as np
import jax
import jax.numpy as jnp
from jax import lax
from jax.experimental import pallas as pl
from jax.experimental.pallas import tpu as pltpu
from jax.sharding import PartitionSpec as P


NACT = 30
VBLK = 48
NBLK = 16
WIDTH = VBLK * NACT
LANES = 128
CORES = 2
CHIPS = 16
BELOW = 2
ABOVE = 3
LONGEST = 10
JOBS = 2
TPAD = 32
PACKED = NACT * TPAD
STEPS = 152
OFFSETS = range(-ABOVE, BELOW + 1)


def swap_plan():
    draw = np.random.default_rng(7)
    first = draw.integers(0, NBLK, STEPS)
    second = (first + draw.integers(1, NBLK, STEPS)) % NBLK
    heat = 0.5 * (0.15 / 0.5) ** (np.arange(STEPS) / STEPS)
    heat[:24] = 4.0
    return (
        np.stack([first, second], axis=1).astype(np.int32).reshape(-1),
        (1.0 / heat).astype(np.float32),
    )


def ring_mask(reach):
    return sum(1 << d for d in range(NBLK) if min(d, NBLK - d) in reach)


def plan_kernel(me, pairs, swaps, coolness, table, words, links, home, load, spots, found, waiting, queue):
    far_base = ring_mask(range(BELOW + ABOVE + 1, NBLK))
    edge_base = ring_mask([BELOW + ABOVE])
    near_edge_base = ring_mask([BELOW + ABOVE - 1])
    shape = (8, 128)

    def turned(base, z):
        return ((base << z) | (base >> (NBLK - z))) & 0xFFFF

    def count(x):
        return lax.population_count(x)

    def clear(z, c):
        links[z] = 0
        load[z] = 0
        return c

    lax.fori_loop(0, NBLK, clear, 0)
    n_pairs = pairs.shape[0] // 2

    def link(d, c):
        p = pairs[2 * d]
        q = pairs[2 * d + 1]
        links[p] = links[p] | (1 << q)
        links[q] = links[q] | (1 << p)
        return c

    lax.fori_loop(0, n_pairs, link, 0)
    cost = jnp.zeros(shape, jnp.int32)
    for z in range(NBLK):
        word = jnp.broadcast_to(links[z] | (z << 16), shape).astype(jnp.int32)
        words[z] = word
        cost = cost + count(word & turned(far_base, z))
    cost = cost // 2
    lane = lax.broadcasted_iota(jnp.int32, shape, 0) * 128 + lax.broadcasted_iota(jnp.int32, shape, 1)
    noise = (lane * 747796405 + 12345) * 1103515245 + 12345

    def step(i, carry):
        cost, noise = carry
        x = swaps[2 * i]
        y = swaps[2 * i + 1]
        wx = words[x]
        wy = words[y]

        def crossed(w):
            t = ((w >> x) ^ (w >> y)) & 1
            return w ^ ((t << x) | (t << y))

        far_x = turned(jnp.int32(far_base), x)
        far_y = turned(jnp.int32(far_base), y)
        change = (
            count(crossed(wy) & far_x)
            + count(crossed(wx) & far_y)
            - count(wx & far_x)
            - count(wy & far_y)
        )
        noise = noise * 1664525 + 1013904223
        chance = ((noise >> 8) & 0xFFFF).astype(jnp.float32) * (1.0 / 65536.0)
        bound = jnp.exp(change.astype(jnp.float32) * (-coolness[i]))
        take = ((change <= 0) | (chance < bound)) & (cost > 0)
        take_bit = take.astype(jnp.int32)
        for z in range(NBLK):
            w = words[z]
            t = ((w >> x) ^ (w >> y)) & take_bit
            words[z] = w ^ ((t << x) | (t << y))
        wx = words[x]
        wy = words[y]
        words[x] = jnp.where(take, wy, wx)
        words[y] = jnp.where(take, wx, wy)
        return cost + change * take_bit, noise

    cost, noise = lax.fori_loop(0, STEPS, step, (cost, noise))
    span_limit = BELOW + ABOVE
    one = jnp.ones(shape, jnp.int32)

    def lap(_, carry):
        slack, late = list(carry[:-1]), carry[-1]
        for chip in range(NBLK):
            y = (chip + BELOW) % NBLK
            for gap in range(span_limit + 1):
                slack[span_limit - gap] = slack[span_limit - gap] + ((words[(y - gap) % NBLK] >> y) & one)
            room = jnp.full(shape, CORES, jnp.int32)
            for k in range(span_limit + 1):
                served = jnp.minimum(slack[k], room)
                slack[k] = slack[k] - served
                room = room - served
            late = late + slack[0]
            slack = slack[1:] + [jnp.zeros(shape, jnp.int32)]
        return (*slack, late)

    nothing = jnp.zeros(shape, jnp.int32)
    late = lax.fori_loop(0, 3, lap, (nothing,) * (span_limit + 2))[-1]
    late = jnp.minimum(late, 1)
    score = jnp.minimum(cost * 2 + late, 8000) * 1024 + lane
    best = jnp.min(score.astype(jnp.float32))
    chosen = score.astype(jnp.float32) == best
    even = best < 1024.0
    for z in range(NBLK):
        w = jnp.sum(jnp.where(chosen, words[z].astype(jnp.float32), 0.0)).astype(jnp.int32)
        home[(w >> 16) & 15] = z

    def span(d):
        x = home[pairs[2 * d]]
        y = home[pairs[2 * d + 1]]
        ahead = (y - x) & (NBLK - 1)
        forward = ahead <= NBLK // 2
        gap = jnp.where(forward, ahead, NBLK - ahead)
        low = jnp.where(forward, y, x) - BELOW
        return gap, low

    def rank(r, c):
        def place(d, c):
            gap, low = span(d)

            def choose(step, best_chip):
                chip = (low + step) & (NBLK - 1)
                better = load[chip] < load[best_chip]
                return jnp.where(better, chip, best_chip)

            now = gap == BELOW + ABOVE - r
            spot = lax.fori_loop(1, jnp.where(now, r + 1, 1), choose, low & (NBLK - 1))

            @pl.when(now)
            def _():
                load[spot] = load[spot] + 1
                spots[d] = spot

            return c

        return lax.fori_loop(0, n_pairs, place, c)

    @pl.when(jnp.logical_not(even))
    def _():
        lax.fori_loop(0, span_limit + 1, rank, 0)

    def empty(i, c):
        found[i] = -1
        waiting[i] = 0
        return c

    def record(d, c):
        x = home[pairs[2 * d]]
        y = home[pairs[2 * d + 1]]
        ahead = (y - x) & (NBLK - 1)
        first = jnp.where(ahead <= NBLK // 2, x, y)
        found[first * 8 + span(d)[0]] = d
        return c

    def serve(c, carry):
        y = (c + BELOW) & (NBLK - 1)
        for gap in range(span_limit + 1):
            d = found[((y - gap) & (NBLK - 1)) * 8 + gap]
            end = c + span_limit - gap

            @pl.when(d >= 0)
            def _(d=d, end=end):
                queue[end * 8 + waiting[end]] = d
                waiting[end] = waiting[end] + 1

        def more(state):
            end, room = state
            return (room > 0) & (end <= c + span_limit)

        def pop(state):
            end, room = state
            some = waiting[end] > 0

            @pl.when(some)
            def _():
                last = waiting[end] - 1
                spots[queue[end * 8 + last]] = c & (NBLK - 1)
                waiting[end] = last

            return jnp.where(some, end, end + 1), jnp.where(some, room - 1, room)

        lax.while_loop(more, pop, (c, jnp.int32(CORES)))
        return carry

    @pl.when(even)
    def _():
        lax.fori_loop(0, NBLK * 8, empty, 0)
        lax.fori_loop(0, n_pairs, record, 0)
        lax.fori_loop(0, 3 * NBLK, serve, 0)

    for j in range(8 * JOBS):
        table[MINE + j] = 0
    table[17] = 0

    def rest(z, c):
        load[z] = 0
        return c

    lax.fori_loop(0, NBLK, rest, 0)

    def settle(d, unfit):
        spot = spots[d] & (NBLK - 1)
        turn = load[spot]
        load[spot] = turn + 1
        table[24 + d] = jnp.minimum((spot * CORES + turn % CORES) * JOBS + turn // CORES, n_pairs * JOBS - 1)

        @pl.when(turn >= CORES)
        def _():
            table[17] = 1

        dp = ((home[pairs[2 * d]] - spot + 8) & 15) - 8
        dq = ((home[pairs[2 * d + 1]] - spot + 8) & 15) - 8

        @pl.when((spot == me[0] // CORES) & (turn < CORES * JOBS))
        def _():
            whose = jnp.where(turn % CORES == me[0] % CORES, MINE, OTHERS)
            slot = whose + 3 * (turn // CORES)
            table[slot] = 1
            table[slot + 1] = dp
            table[slot + 2] = dq

        within = (dp >= -ABOVE) & (dp <= BELOW) & (dq >= -ABOVE) & (dq <= BELOW) & (turn < CORES * JOBS)
        return unfit + jnp.where(within, 0, 1)

    unfit = lax.fori_loop(0, n_pairs, settle, 0)
    table[0] = jnp.where(unfit == 0, 1, 0)

    @pl.when(unfit > 0)
    def _():
        table[17] = 0
        for j in range(8 * JOBS):
            table[MINE + j] = 0

    for z in range(NBLK):
        table[1 + z] = home[z]


def make_plan(me, pair_blocks):
    swaps, coolness = swap_plan()
    smem = pl.BlockSpec(memory_space=pltpu.SMEM)
    return pl.pallas_call(
        plan_kernel,
        out_shape=jax.ShapeDtypeStruct((96,), jnp.int32),
        in_specs=[smem] * 4,
        out_specs=smem,
        scratch_shapes=[
            pltpu.VMEM((NBLK, 8, 128), jnp.int32),
            pltpu.SMEM((NBLK,), jnp.int32),
            pltpu.SMEM((NBLK,), jnp.int32),
            pltpu.SMEM((NBLK,), jnp.int32),
            pltpu.SMEM((pair_blocks.shape[0],), jnp.int32),
            pltpu.SMEM((NBLK * 8,), jnp.int32),
            pltpu.SMEM((NBLK * 8,), jnp.int32),
            pltpu.SMEM((NBLK * 8 * 8,), jnp.int32),
        ],
        name="plan",
    )(me, pair_blocks.reshape(-1), jnp.asarray(swaps), jnp.asarray(coolness))


PER_STEP = 4


def pack_kernel(me, table, slab, *rest):
    outs = rest[: 2 * LONGEST]
    turned, packed, sems = rest[2 * LONGEST :]
    g = pl.program_id(0)
    chip = me[0] // CORES
    rows = slab.shape[0]

    def copies(b):
        o = ((table[1 + b] - chip + 8) & 15) - 8
        for reach in range(1, LONGEST + 1):
            yield o == reach - ABOVE, pltpu.make_async_copy(packed.at[b], outs[reach - 1], sems.at[reach - 1])
            yield o == BELOW - reach, pltpu.make_async_copy(
                packed.at[b], outs[LONGEST + reach - 1], sems.at[LONGEST + reach - 1]
            )

    for i in range(PER_STEP):
        b = g * PER_STEP + i
        part = slab[:, i * WIDTH : (i + 1) * WIDTH].astype(jnp.float32)
        part = jnp.concatenate([part, jnp.zeros((LANES - rows, WIDTH), jnp.float32)], axis=0)
        turned[...] = part.T
        for t in range(NACT):
            packed[b, t * VBLK : (t + 1) * VBLK, :] = turned[pl.ds(t, VBLK, stride=NACT), :].astype(jnp.bfloat16)
        for when, copy in copies(b):

            @pl.when(when)
            def _(copy=copy):
                copy.start()

    @pl.when(g == NBLK // PER_STEP - 1)
    def _():
        for n in range(2 * LONGEST):
            pltpu.make_async_copy(packed.at[0], outs[n], sems.at[n]).wait()


def pack(me, table, slabs):
    rows = slabs.shape[0]
    smem = pl.BlockSpec(memory_space=pltpu.SMEM)
    return pl.pallas_call(
        pack_kernel,
        grid=(NBLK // PER_STEP,),
        in_specs=[smem, smem, pl.BlockSpec((rows, PER_STEP * WIDTH), lambda g: (0, g))],
        out_specs=[pl.BlockSpec(memory_space=pl.ANY)] * (2 * LONGEST),
        out_shape=[jax.ShapeDtypeStruct((WIDTH, LANES), jnp.bfloat16)] * (2 * LONGEST),
        scratch_shapes=[
            pltpu.VMEM((WIDTH, LANES), jnp.float32),
            pltpu.VMEM((NBLK, WIDTH, LANES), jnp.bfloat16),
            pltpu.SemaphoreType.DMA((2 * LONGEST,)),
        ],
        compiler_params=pltpu.CompilerParams(vmem_limit_bytes=40 * 1024 * 1024),
        name="pack",
    )(me, table, slabs)


ROW_TILE = 480
TILES = -(-WIDTH // LANES)
COL_TILES = ((0, 512), (512, 512), (1024, 416))
GROUP = 8
HBM = pltpu.MemorySpace.HBM
MINE = 64
OTHERS = 72


def unflatten(refs, keys):
    refs = list(refs)
    return [{d: refs.pop(0) for d in offsets} for offsets in keys]


def flatten(pieces, keys, sources):
    return [pieces[s][d] for s, offsets in zip(sources, keys) for d in offsets]


def keys_of(pieces, sources):
    return [sorted(pieces[s]) for s in sources]


def held_here(wanted, offsets):
    if len(offsets) == len(OFFSETS):
        return None
    here = wanted == min(offsets)
    for d in sorted(offsets)[1:]:
        here = here | (wanted == d)
    return here


def select_kernel(table, *rest, keys, sources, job):
    count = sum(map(len, keys))
    pieces = unflatten(rest[:count], keys)
    out, held, sems, out_sem = rest[count:]

    @pl.when(table[OTHERS + 3 * job] == 1)
    def _():
        for side in range(2):
            wanted = table[OTHERS + 3 * job + 1 + side]
            for n in range(len(sources)):
                for d, piece in pieces[n].items():

                    @pl.when(wanted == d)
                    def _(piece=piece, n=n, side=side):
                        pltpu.make_async_copy(piece, held.at[side, n], sems.at[side, n]).start()

        for side in range(2):
            wanted = table[OTHERS + 3 * job + 1 + side]
            for n in range(len(sources)):
                here = held_here(wanted, pieces[n])
                piece = next(iter(pieces[n].values()))

                def pass_on(piece=piece, side=side, n=n):
                    pltpu.make_async_copy(piece, held.at[side, n], sems.at[side, n]).wait()
                    pltpu.make_async_copy(held.at[side, n], out.at[side, n], out_sem.at[side, n]).start()

                pass_on() if here is None else pl.when(here)(pass_on)
        for side in range(2):
            wanted = table[OTHERS + 3 * job + 1 + side]
            for n in range(len(sources)):
                here = held_here(wanted, pieces[n])

                def close(side=side, n=n):
                    pltpu.make_async_copy(held.at[side, n], out.at[side, n], out_sem.at[side, n]).wait()

                close() if here is None else pl.when(here)(close)


def select(table, pieces, sources, job):
    keys = keys_of(pieces, sources)
    flat = flatten(pieces, keys, sources)
    n = len(sources)
    return pl.pallas_call(
        lambda *refs: select_kernel(*refs, keys=keys, sources=sources, job=job),
        in_specs=[pl.BlockSpec(memory_space=pltpu.SMEM)] + [pl.BlockSpec(memory_space=HBM)] * len(flat),
        out_specs=pl.BlockSpec(memory_space=HBM),
        out_shape=jax.ShapeDtypeStruct((2, n, WIDTH, LANES), jnp.bfloat16),
        scratch_shapes=[
            pltpu.VMEM((2, n, WIDTH, LANES), jnp.bfloat16),
            pltpu.SemaphoreType.DMA((2, n)),
            pltpu.SemaphoreType.DMA((2, n)),
        ],
        name="select",
    )(table, *flat)


def multiply(table, job, pieces, other, late, bufs, sems, acc, fresh, ready=None):
    def lanes(n, who):
        return pl.ds((n * CORES + who) * LANES, LANES)

    for side, buf in enumerate(bufs):
        wanted = table[MINE + 3 * job + 1 + side]
        for n in range(len(pieces)):
            sources = [(None, other.at[side, n], 1)] if not late[n] else []
            if late[n]:
                waits = held_here(wanted, late[n])
                sources.append((jnp.logical_not(waits), other.at[side, n], 1))
                sources += [(wanted == d, piece, 1) for d, piece in late[n].items()]
            sources += [(wanted == d, piece, 0) for d, piece in pieces[n].items()]
            for when, piece, who in sources:

                def begin(piece=piece, n=n, side=side, buf=buf, who=who):
                    pltpu.make_async_copy(piece, buf.at[:, lanes(n, who)], sems.at[side, n, who]).start()

                begin() if when is None else pl.when(when)(begin)

    for side, buf in enumerate(bufs):
        for n in range(len(pieces)):
            for who in range(CORES):
                pltpu.make_async_copy(other.at[side, n], buf.at[:, lanes(n, who)], sems.at[side, n, who]).wait()
    col_buf, row_buf = bufs
    if ready is not None:
        ready.wait()

    def rows(m, c):
        here = pl.ds(pl.multiple_of(m * ROW_TILE, ROW_TILE), ROW_TILE)
        left = row_buf[here, :]
        for start, size in COL_TILES:
            part = lax.dot_general(
                left, col_buf[start : start + size, :], (((1,), (1,)), ((), ())), preferred_element_type=jnp.float32
            )
            for at in range(0, size, LANES):
                wide = min(LANES, size - at)
                tile = acc.at[(start + at) // LANES, here, pl.ds(0, wide)]
                if fresh:
                    tile[...] = part[:, at : at + wide]
                else:
                    tile[...] += part[:, at : at + wide]
        return c

    lax.fori_loop(0, WIDTH // ROW_TILE, rows, 0)


def early_kernel(table, other, *rest, keys, job, fresh):
    before = None
    if not fresh:
        before, *rest = rest
    count = sum(map(len, keys))
    pieces = unflatten(rest[:count], keys)
    out, col_buf, row_buf, acc, sems, sem = rest[count:]

    @pl.when(table[MINE + 3 * job] == 1)
    def _():
        ready = None
        if not fresh:
            ready = pltpu.make_async_copy(before, acc, sem)
            ready.start()
        late = [{} for _ in keys]
        multiply(table, job, pieces, other, late, (col_buf, row_buf), sems, acc, fresh, ready)
        copy = pltpu.make_async_copy(acc, out, sem)
        copy.start()
        copy.wait()


def density_kernel(rdm, out, wide, lifted):
    out[...] = jnp.zeros(out.shape, out.dtype)
    lifted[...] = jnp.zeros(lifted.shape, jnp.float32)
    wide[...] = rdm[...].astype(jnp.float32)
    for v in range(NACT):
        lifted[:, v * TPAD : v * TPAD + NACT] = wide[:, v * NACT : (v + 1) * NACT]
    for t in range(NACT):
        out[t * TPAD : t * TPAD + NACT, :] = lifted[t * NACT : (t + 1) * NACT, :].astype(jnp.bfloat16)


def spread_density(rdm):
    order = NACT * NACT
    return pl.pallas_call(
        density_kernel,
        out_shape=jax.ShapeDtypeStruct((PACKED, PACKED), jnp.bfloat16),
        scratch_shapes=[pltpu.VMEM((order, order), jnp.float32), pltpu.VMEM((order, PACKED), jnp.float32)],
        name="density",
    )(rdm)


def finish_kernel(table, other, before, density, *rest, keys, late_keys, job):
    count = sum(map(len, keys))
    pieces = unflatten(rest[:count], keys)
    rest = rest[count:]
    count = sum(map(len, late_keys))
    late = unflatten(rest[:count], late_keys)
    out, col_buf, row_buf, acc, spread, sems, sem = rest[count:]

    @pl.when(table[MINE + 3 * job] == 0)
    def _():
        out[...] = jnp.zeros(out.shape, out.dtype)

    @pl.when(table[MINE + 3 * job] == 1)
    def _():
        copy = pltpu.make_async_copy(before, acc.at[:, pl.ds(0, WIDTH), :], sem)
        copy.start()
        acc[:, WIDTH:, :] = jnp.zeros((TILES, acc.shape[1] - WIDTH, LANES), jnp.float32)
        multiply(table, job, pieces, other, late, (col_buf, row_buf), sems, acc, False, copy)

        def group(g, carry):
            for i in range(GROUP):
                here = pl.ds(g * GROUP + i, TPAD, stride=VBLK)
                rows = jnp.concatenate([acc[c, here, :] for c in range(TILES)], axis=1).astype(jnp.bfloat16)
                for t in range(NACT):
                    spread[t * TPAD : (t + 1) * TPAD, i * VBLK : (i + 1) * VBLK] = rows[:, t * VBLK : (t + 1) * VBLK]
            x = spread[...]
            y = jnp.dot(density[...], x, preferred_element_type=jnp.float32)
            out[pl.ds(g, 1), :] = jnp.sum(y * x.astype(jnp.float32), axis=0, keepdims=True)
            return carry

        lax.fori_loop(0, VBLK // GROUP, group, 0)


def product_scratch(sources, rows):
    depth = len(sources) * CORES * LANES
    return [
        pltpu.VMEM((WIDTH, depth), jnp.bfloat16),
        pltpu.VMEM((WIDTH, depth), jnp.bfloat16),
        pltpu.VMEM((TILES, rows, LANES), jnp.float32),
    ]


ROOM = pltpu.CompilerParams(vmem_limit_bytes=48 * 1024 * 1024)


def early(table, other, before, pieces, sources, job):
    keys = keys_of(pieces, sources)
    flat = flatten(pieces, keys, sources)
    fresh = before is None
    held = [] if fresh else [before]
    in_hbm = pl.BlockSpec(memory_space=HBM)
    return pl.pallas_call(
        lambda *refs: early_kernel(*refs, keys=keys, job=job, fresh=fresh),
        in_specs=[pl.BlockSpec(memory_space=pltpu.SMEM)] + [in_hbm] * (1 + len(held) + len(flat)),
        out_specs=in_hbm,
        out_shape=jax.ShapeDtypeStruct((TILES, WIDTH, LANES), jnp.float32),
        scratch_shapes=product_scratch(sources, WIDTH)
        + [pltpu.SemaphoreType.DMA((2, len(sources), CORES)), pltpu.SemaphoreType.DMA],
        compiler_params=ROOM,
        name="early",
    )(table, other, *held, *flat)


def finish(table, other, before, density, pieces, late, sources, job):
    keys = keys_of(pieces, sources)
    late_keys = keys_of(late, sources)
    flat = flatten(pieces, keys, sources) + flatten(late, late_keys, sources)
    in_hbm = pl.BlockSpec(memory_space=HBM)
    return pl.pallas_call(
        lambda *refs: finish_kernel(*refs, keys=keys, late_keys=late_keys, job=job),
        in_specs=[pl.BlockSpec(memory_space=pltpu.SMEM), in_hbm, in_hbm, pl.BlockSpec(memory_space=pltpu.VMEM)]
        + [in_hbm] * len(flat),
        out_specs=pl.BlockSpec(memory_space=pltpu.VMEM),
        out_shape=jax.ShapeDtypeStruct((VBLK // GROUP, GROUP * VBLK), jnp.float32),
        scratch_shapes=product_scratch(sources, VBLK * TPAD)
        + [
            pltpu.VMEM((PACKED, GROUP * VBLK), jnp.bfloat16),
            pltpu.SemaphoreType.DMA((2, len(sources), CORES)),
            pltpu.SemaphoreType.DMA,
        ],
        compiler_params=ROOM,
        name="finish",
    )(table, other, before, density, *flat)


def ring_shift(hops):
    n = lax.axis_size("aux")
    return [(i, (i + hops * CORES) % n) for i in range(n)]


def to_other_core(x):
    n = lax.axis_size("aux")
    return lax.ppermute(x, "aux", [(i, i ^ 1) for i in range(n)])


def energies_of(paired, orbital_energy, pair_blocks):
    table = orbital_energy.reshape(NBLK, VBLK)
    rows = table[pair_blocks[:, 0]]
    cols = table[pair_blocks[:, 1]]
    energy = -paired / (rows[:, :, None] + cols[:, None, :])
    weight = jnp.where(pair_blocks[:, 0] == pair_blocks[:, 1], jnp.float32(1.0), jnp.float32(2.0))
    total = jnp.sum(weight * jnp.sum(energy, axis=(1, 2)))
    mine = lax.dynamic_index_in_dim(energy, lax.axis_index("aux"), 0, keepdims=False)
    mean_energy = total / (VBLK * VBLK * lax.axis_size("aux"))
    return mine, mean_energy.reshape(1)


def sources_within(low, high):
    return [s for s in range(-CHIPS // 2, CHIPS // 2) if low <= abs(s) <= high]


NEAREST = sources_within(0, 3)
NEAR = sources_within(4, 5)
FAR = sources_within(6, CHIPS)


LAST_SELECTED = 8


def both_cores(x):
    core = lax.axis_index("aux") % CORES
    other = to_other_core(x)
    return jnp.where(core == 0, jnp.stack([x, other]), jnp.stack([other, x]))


def of_everyone(x):
    n = lax.axis_size("aux")
    rings = [list(range(core, n, CORES)) for core in range(CORES)]
    chips = lax.all_gather(both_cores(x), "aux", axis_index_groups=rings)
    return chips.reshape(n, VBLK, VBLK)


def planned(table, me, slabs, rdm, orbital_energy, pair_blocks):
    sent = pack(me, table, slabs)
    pieces = {s: {} for s in range(-CHIPS // 2, CHIPS // 2)}
    late = {s: {} for s in range(-CHIPS // 2, CHIPS // 2)}

    def keep(source, offset, value, hop):
        source = (source + CHIPS // 2) % CHIPS - CHIPS // 2
        if -ABOVE <= offset <= BELOW:
            pieces[source][offset] = value
            if hop > LAST_SELECTED:
                late[source][offset] = to_other_core(value)

    right = {reach: sent[reach - 1] for reach in range(1, LONGEST + 1)}
    left = {reach: sent[LONGEST + reach - 1] for reach in range(1, LONGEST + 1)}
    for offset in OFFSETS:
        keep(0, offset, right[offset + ABOVE] if offset > -ABOVE else left[BELOW + ABOVE], 0)
    none_late = {s: {} for s in pieces}

    def exchange(pieces, sources, job):
        chosen = select(table, pieces, sources, job)
        return to_other_core(chosen)

    for hop in range(1, LONGEST + 1):
        for reach in range(LONGEST, hop - 1, -1):
            right[reach] = lax.ppermute(right[reach], "aux", ring_shift(1))
            left[reach] = lax.ppermute(left[reach], "aux", ring_shift(-1))
            keep(-hop, reach - ABOVE - hop, right[reach], hop)
            keep(hop, BELOW - reach + hop, left[reach], hop)
        if hop == 1:
            density = spread_density(rdm)
        if hop == 3:
            other = exchange(pieces, NEAREST, 0)
            sums = early(table, other, None, pieces, NEAREST, 0)
        if hop == 5:
            other = exchange(pieces, NEAR, 0)
            sums = early(table, other, sums, pieces, NEAR, 0)
        if hop == LAST_SELECTED:
            other = exchange(pieces, FAR, 0)
    paired = finish(table, other, sums, density, pieces, late, FAR, 0)

    def second_job(pieces):
        other = exchange(pieces, NEAREST, 1)
        sums = early(table, other, None, pieces, NEAREST, 1)
        other = exchange(pieces, NEAR, 1)
        sums = early(table, other, sums, pieces, NEAR, 1)
        other = exchange(pieces, FAR, 1)
        return of_everyone(finish(table, other, sums, density, pieces, none_late, FAR, 1))

    paired = of_everyone(paired)
    extra = lax.cond(table[17] == 1, second_job, lambda pieces: jnp.zeros_like(paired), pieces)
    everyone = jnp.stack([paired, extra], axis=1).reshape(-1, VBLK, VBLK)
    paired = everyone[lax.dynamic_slice_in_dim(table, 24, pair_blocks.shape[0])].transpose(0, 2, 1)
    return energies_of(paired, orbital_energy, pair_blocks)


def unplanned(table, me, slabs, rdm, orbital_energy, pair_blocks):
    local_rows = slabs.shape[0]
    blocked = slabs.reshape(local_rows, NBLK, WIDTH)
    sides = []
    for side in range(2):
        outgoing = jnp.take(blocked, pair_blocks[:, side], axis=1)
        arrived = lax.all_to_all(outgoing, "aux", split_axis=1, concat_axis=0, tiled=True)
        sides.append(arrived.reshape(-1, WIDTH))
    products = lax.dot_general(sides[0], sides[1], (((0,), (0,)), ((), ())), preferred_element_type=jnp.float32)
    reordered = (
        products.astype(jnp.bfloat16)
        .reshape(VBLK, NACT, VBLK, NACT)
        .transpose(0, 2, 1, 3)
        .reshape(VBLK * VBLK, NACT * NACT)
    )
    contracted = jnp.dot(reordered, rdm, preferred_element_type=jnp.float32)
    paired = jnp.sum(contracted * reordered.astype(jnp.float32), axis=1).reshape(VBLK, VBLK)
    return energies_of(lax.all_gather(paired, "aux"), orbital_energy, pair_blocks)


def per_device(slabs, rdm, orbital_energy, pair_blocks):
    me = lax.axis_index("aux").reshape(1).astype(jnp.int32)
    table = make_plan(me, pair_blocks)
    given = (table, me, slabs, rdm, orbital_energy, pair_blocks)
    results = planned(*given)
    return lax.cond(table[0] == 1, lambda *_: results, unplanned, *given)


def solution(mesh):
    return jax.shard_map(
        per_device,
        mesh=mesh,
        in_specs=(P(("groups", "aux"), None), P("groups", None), P("groups"), P("groups", None)),
        out_specs=(P(("groups", "aux"), None), P("groups")),
        check_vma=False,
    )
```

```python
import numpy as np
import jax
import jax.numpy as jnp
from jax import lax
from jax.experimental import pallas as pl
from jax.experimental.pallas import tpu as pltpu
from jax.sharding import PartitionSpec as P


NACT = 30
VBLK = 48
NBLK = 16
WIDTH = VBLK * NACT
LANES = 128
CORES = 2
CHIPS = 16
BELOW = 2
ABOVE = 3
LONGEST = 10
JOBS = 2
TPAD = 32
PACKED = NACT * TPAD
STEPS = 144
OFFSETS = range(-ABOVE, BELOW + 1)


def swap_plan():
    draw = np.random.default_rng(7)
    first = draw.integers(0, NBLK, STEPS)
    second = (first + draw.integers(1, NBLK, STEPS)) % NBLK
    heat = 0.5 * (0.15 / 0.5) ** (np.arange(STEPS) / STEPS)
    heat[:12] = 4.0
    return (
        np.stack([first, second], axis=1).astype(np.int32).reshape(-1),
        (1.0 / heat).astype(np.float32),
    )


def ring_mask(reach):
    return sum(1 << d for d in range(NBLK) if min(d, NBLK - d) in reach)


def plan_kernel(me, pairs, swaps, coolness, table, words, links, home, load, spots, found, waiting, queue):
    far_base = ring_mask(range(BELOW + ABOVE + 1, NBLK))
    edge_base = ring_mask([BELOW + ABOVE])
    near_edge_base = ring_mask([BELOW + ABOVE - 1])
    shape = (8, 128)

    def turned(base, z):
        return ((base << z) | (base >> (NBLK - z))) & 0xFFFF

    def count(x):
        return lax.population_count(x)

    def clear(z, c):
        links[z] = 0
        load[z] = 0
        return c

    lax.fori_loop(0, NBLK, clear, 0)
    n_pairs = pairs.shape[0] // 2

    def link(d, c):
        p = pairs[2 * d]
        q = pairs[2 * d + 1]
        links[p] = links[p] | (1 << q)
        links[q] = links[q] | (1 << p)
        return c

    lax.fori_loop(0, n_pairs, link, 0)
    cost = jnp.zeros(shape, jnp.int32)
    for z in range(NBLK):
        word = jnp.broadcast_to(links[z] | (z << 16), shape).astype(jnp.int32)
        words[z] = word
        cost = cost + count(word & turned(far_base, z))
    cost = cost // 2
    lane = lax.broadcasted_iota(jnp.int32, shape, 0) * 128 + lax.broadcasted_iota(jnp.int32, shape, 1)
    noise = (lane * 747796405 + 12345) * 1103515245 + 12345

    def step(i, carry):
        cost, noise = carry
        x = swaps[2 * i]
        y = swaps[2 * i + 1]
        wx = words[x]
        wy = words[y]

        def crossed(w):
            t = ((w >> x) ^ (w >> y)) & 1
            return w ^ ((t << x) | (t << y))

        far_x = turned(jnp.int32(far_base), x)
        far_y = turned(jnp.int32(far_base), y)
        change = (
            count(crossed(wy) & far_x)
            + count(crossed(wx) & far_y)
            - count(wx & far_x)
            - count(wy & far_y)
        )
        noise = noise * 1664525 + 1013904223
        chance = ((noise >> 8) & 0xFFFF).astype(jnp.float32) * (1.0 / 65536.0)
        bound = jnp.exp(change.astype(jnp.float32) * (-coolness[i]))
        take = ((change <= 0) | (chance < bound)) & (cost > 0)
        take_bit = take.astype(jnp.int32)
        for z in range(NBLK):
            w = words[z]
            t = ((w >> x) ^ (w >> y)) & take_bit
            words[z] = w ^ ((t << x) | (t << y))
        wx = words[x]
        wy = words[y]
        words[x] = jnp.where(take, wy, wx)
        words[y] = jnp.where(take, wx, wy)
        return cost + change * take_bit, noise

    cost, noise = lax.fori_loop(0, STEPS, step, (cost, noise))
    span_limit = BELOW + ABOVE
    one = jnp.ones(shape, jnp.int32)

    def lap(_, carry):
        slack, late = list(carry[:-1]), carry[-1]
        for chip in range(NBLK):
            y = (chip + BELOW) % NBLK
            for gap in range(span_limit + 1):
                slack[span_limit - gap] = slack[span_limit - gap] + ((words[(y - gap) % NBLK] >> y) & one)
            room = jnp.full(shape, CORES, jnp.int32)
            for k in range(span_limit + 1):
                served = jnp.minimum(slack[k], room)
                slack[k] = slack[k] - served
                room = room - served
            late = late + slack[0]
            slack = slack[1:] + [jnp.zeros(shape, jnp.int32)]
        return (*slack, late)

    nothing = jnp.zeros(shape, jnp.int32)
    late = lax.fori_loop(0, 3, lap, (nothing,) * (span_limit + 2))[-1]
    late = jnp.minimum(late, 1)
    score = jnp.minimum(cost * 2 + late, 8000) * 1024 + lane
    best = jnp.min(score.astype(jnp.float32))
    chosen = score.astype(jnp.float32) == best
    even = best < 1024.0
    for z in range(NBLK):
        w = jnp.sum(jnp.where(chosen, words[z].astype(jnp.float32), 0.0)).astype(jnp.int32)
        home[(w >> 16) & 15] = z

    def span(d):
        x = home[pairs[2 * d]]
        y = home[pairs[2 * d + 1]]
        ahead = (y - x) & (NBLK - 1)
        forward = ahead <= NBLK // 2
        gap = jnp.where(forward, ahead, NBLK - ahead)
        low = jnp.where(forward, y, x) - BELOW
        return gap, low

    def rank(r, c):
        def place(d, c):
            gap, low = span(d)

            def choose(step, best_chip):
                chip = (low + step) & (NBLK - 1)
                better = load[chip] < load[best_chip]
                return jnp.where(better, chip, best_chip)

            now = gap == BELOW + ABOVE - r
            spot = lax.fori_loop(1, jnp.where(now, r + 1, 1), choose, low & (NBLK - 1))

            @pl.when(now)
            def _():
                load[spot] = load[spot] + 1
                spots[d] = spot

            return c

        return lax.fori_loop(0, n_pairs, place, c)

    @pl.when(jnp.logical_not(even))
    def _():
        lax.fori_loop(0, span_limit + 1, rank, 0)

    def empty(i, c):
        found[i] = -1
        waiting[i] = 0
        return c

    def record(d, c):
        x = home[pairs[2 * d]]
        y = home[pairs[2 * d + 1]]
        ahead = (y - x) & (NBLK - 1)
        first = jnp.where(ahead <= NBLK // 2, x, y)
        found[first * 8 + span(d)[0]] = d
        return c

    def serve(c, carry):
        y = (c + BELOW) & (NBLK - 1)
        for gap in range(span_limit + 1):
            d = found[((y - gap) & (NBLK - 1)) * 8 + gap]
            end = c + span_limit - gap

            @pl.when(d >= 0)
            def _(d=d, end=end):
                queue[end * 8 + waiting[end]] = d
                waiting[end] = waiting[end] + 1

        def more(state):
            end, room = state
            return (room > 0) & (end <= c + span_limit)

        def pop(state):
            end, room = state
            some = waiting[end] > 0

            @pl.when(some)
            def _():
                last = waiting[end] - 1
                spots[queue[end * 8 + last]] = c & (NBLK - 1)
                waiting[end] = last

            return jnp.where(some, end, end + 1), jnp.where(some, room - 1, room)

        lax.while_loop(more, pop, (c, jnp.int32(CORES)))
        return carry

    @pl.when(even)
    def _():
        lax.fori_loop(0, NBLK * 8, empty, 0)
        lax.fori_loop(0, n_pairs, record, 0)
        lax.fori_loop(0, 3 * NBLK, serve, 0)

    for j in range(8 * JOBS):
        table[MINE + j] = 0
    table[17] = 0

    def rest(z, c):
        load[z] = 0
        return c

    lax.fori_loop(0, NBLK, rest, 0)

    def settle(d, unfit):
        spot = spots[d] & (NBLK - 1)
        turn = load[spot]
        load[spot] = turn + 1
        table[24 + d] = jnp.minimum((spot * CORES + turn % CORES) * JOBS + turn // CORES, n_pairs * JOBS - 1)

        @pl.when(turn >= CORES)
        def _():
            table[17] = 1

        dp = ((home[pairs[2 * d]] - spot + 8) & 15) - 8
        dq = ((home[pairs[2 * d + 1]] - spot + 8) & 15) - 8

        @pl.when((spot == me[0] // CORES) & (turn < CORES * JOBS))
        def _():
            whose = jnp.where(turn % CORES == me[0] % CORES, MINE, OTHERS)
            slot = whose + 3 * (turn // CORES)
            table[slot] = 1
            table[slot + 1] = dp
            table[slot + 2] = dq

        within = (dp >= -ABOVE) & (dp <= BELOW) & (dq >= -ABOVE) & (dq <= BELOW) & (turn < CORES * JOBS)
        return unfit + jnp.where(within, 0, 1)

    unfit = lax.fori_loop(0, n_pairs, settle, 0)
    table[0] = jnp.where(unfit == 0, 1, 0)

    @pl.when(unfit > 0)
    def _():
        table[17] = 0
        for j in range(8 * JOBS):
            table[MINE + j] = 0

    for z in range(NBLK):
        table[1 + z] = home[z]


def make_plan(me, pair_blocks):
    swaps, coolness = swap_plan()
    smem = pl.BlockSpec(memory_space=pltpu.SMEM)
    return pl.pallas_call(
        plan_kernel,
        out_shape=jax.ShapeDtypeStruct((96,), jnp.int32),
        in_specs=[smem] * 4,
        out_specs=smem,
        scratch_shapes=[
            pltpu.VMEM((NBLK, 8, 128), jnp.int32),
            pltpu.SMEM((NBLK,), jnp.int32),
            pltpu.SMEM((NBLK,), jnp.int32),
            pltpu.SMEM((NBLK,), jnp.int32),
            pltpu.SMEM((pair_blocks.shape[0],), jnp.int32),
            pltpu.SMEM((NBLK * 8,), jnp.int32),
            pltpu.SMEM((NBLK * 8,), jnp.int32),
            pltpu.SMEM((NBLK * 8 * 8,), jnp.int32),
        ],
        name="plan",
    )(me, pair_blocks.reshape(-1), jnp.asarray(swaps), jnp.asarray(coolness))


PER_STEP = 4


def pack_kernel(me, table, slab, *rest):
    outs = rest[: 2 * LONGEST]
    turned, packed, sems = rest[2 * LONGEST :]
    g = pl.program_id(0)
    chip = me[0] // CORES
    rows = slab.shape[0]

    def copies(b):
        o = ((table[1 + b] - chip + 8) & 15) - 8
        for reach in range(1, LONGEST + 1):
            yield o == reach - ABOVE, pltpu.make_async_copy(packed.at[b], outs[reach - 1], sems.at[reach - 1])
            yield o == BELOW - reach, pltpu.make_async_copy(
                packed.at[b], outs[LONGEST + reach - 1], sems.at[LONGEST + reach - 1]
            )

    for i in range(PER_STEP):
        b = g * PER_STEP + i
        part = slab[:, i * WIDTH : (i + 1) * WIDTH].astype(jnp.float32)
        part = jnp.concatenate([part, jnp.zeros((LANES - rows, WIDTH), jnp.float32)], axis=0)
        turned[...] = part.T
        for t in range(NACT):
            packed[b, t * VBLK : (t + 1) * VBLK, :] = turned[pl.ds(t, VBLK, stride=NACT), :].astype(jnp.bfloat16)
        for when, copy in copies(b):

            @pl.when(when)
            def _(copy=copy):
                copy.start()

    @pl.when(g == NBLK // PER_STEP - 1)
    def _():
        for n in range(2 * LONGEST):
            pltpu.make_async_copy(packed.at[0], outs[n], sems.at[n]).wait()


def pack(me, table, slabs):
    rows = slabs.shape[0]
    smem = pl.BlockSpec(memory_space=pltpu.SMEM)
    return pl.pallas_call(
        pack_kernel,
        grid=(NBLK // PER_STEP,),
        in_specs=[smem, smem, pl.BlockSpec((rows, PER_STEP * WIDTH), lambda g: (0, g))],
        out_specs=[pl.BlockSpec(memory_space=pl.ANY)] * (2 * LONGEST),
        out_shape=[jax.ShapeDtypeStruct((WIDTH, LANES), jnp.bfloat16)] * (2 * LONGEST),
        scratch_shapes=[
            pltpu.VMEM((WIDTH, LANES), jnp.float32),
            pltpu.VMEM((NBLK, WIDTH, LANES), jnp.bfloat16),
            pltpu.SemaphoreType.DMA((2 * LONGEST,)),
        ],
        compiler_params=pltpu.CompilerParams(vmem_limit_bytes=40 * 1024 * 1024),
        name="pack",
    )(me, table, slabs)


ROW_TILE = 480
TILES = -(-WIDTH // LANES)
COL_TILES = ((0, 512), (512, 512), (1024, 416))
GROUP = 8
HBM = pltpu.MemorySpace.HBM
MINE = 64
OTHERS = 72


def unflatten(refs, keys):
    refs = list(refs)
    return [{d: refs.pop(0) for d in offsets} for offsets in keys]


def flatten(pieces, keys, sources):
    return [pieces[s][d] for s, offsets in zip(sources, keys) for d in offsets]


def keys_of(pieces, sources):
    return [sorted(pieces[s]) for s in sources]


def held_here(wanted, offsets):
    if len(offsets) == len(OFFSETS):
        return None
    here = wanted == min(offsets)
    for d in sorted(offsets)[1:]:
        here = here | (wanted == d)
    return here


def select_kernel(table, *rest, keys, sources, job):
    count = sum(map(len, keys))
    pieces = unflatten(rest[:count], keys)
    out, held, sems, out_sem = rest[count:]

    @pl.when(table[OTHERS + 3 * job] == 1)
    def _():
        for side in range(2):
            wanted = table[OTHERS + 3 * job + 1 + side]
            for n in range(len(sources)):
                for d, piece in pieces[n].items():

                    @pl.when(wanted == d)
                    def _(piece=piece, n=n, side=side):
                        pltpu.make_async_copy(piece, held.at[side, n], sems.at[side, n]).start()

        for side in range(2):
            wanted = table[OTHERS + 3 * job + 1 + side]
            for n in range(len(sources)):
                here = held_here(wanted, pieces[n])
                piece = next(iter(pieces[n].values()))

                def pass_on(piece=piece, side=side, n=n):
                    pltpu.make_async_copy(piece, held.at[side, n], sems.at[side, n]).wait()
                    pltpu.make_async_copy(held.at[side, n], out.at[side, n], out_sem.at[side, n]).start()

                pass_on() if here is None else pl.when(here)(pass_on)
        for side in range(2):
            wanted = table[OTHERS + 3 * job + 1 + side]
            for n in range(len(sources)):
                here = held_here(wanted, pieces[n])

                def close(side=side, n=n):
                    pltpu.make_async_copy(held.at[side, n], out.at[side, n], out_sem.at[side, n]).wait()

                close() if here is None else pl.when(here)(close)


def select(table, pieces, sources, job):
    keys = keys_of(pieces, sources)
    flat = flatten(pieces, keys, sources)
    n = len(sources)
    return pl.pallas_call(
        lambda *refs: select_kernel(*refs, keys=keys, sources=sources, job=job),
        in_specs=[pl.BlockSpec(memory_space=pltpu.SMEM)] + [pl.BlockSpec(memory_space=HBM)] * len(flat),
        out_specs=pl.BlockSpec(memory_space=HBM),
        out_shape=jax.ShapeDtypeStruct((2, n, WIDTH, LANES), jnp.bfloat16),
        scratch_shapes=[
            pltpu.VMEM((2, n, WIDTH, LANES), jnp.bfloat16),
            pltpu.SemaphoreType.DMA((2, n)),
            pltpu.SemaphoreType.DMA((2, n)),
        ],
        name="select",
    )(table, *flat)


def multiply(table, job, pieces, other, late, bufs, sems, acc, fresh, ready=None, meanwhile=None):
    def lanes(n, who):
        return pl.ds((n * CORES + who) * LANES, LANES)

    for side, buf in enumerate(bufs):
        wanted = table[MINE + 3 * job + 1 + side]
        for n in range(len(pieces)):
            sources = [(None, other.at[side, n], 1)] if not late[n] else []
            if late[n]:
                waits = held_here(wanted, late[n])
                sources.append((jnp.logical_not(waits), other.at[side, n], 1))
                sources += [(wanted == d, piece, 1) for d, piece in late[n].items()]
            sources += [(wanted == d, piece, 0) for d, piece in pieces[n].items()]
            for when, piece, who in sources:

                def begin(piece=piece, n=n, side=side, buf=buf, who=who):
                    pltpu.make_async_copy(piece, buf.at[:, lanes(n, who)], sems.at[side, n, who]).start()

                begin() if when is None else pl.when(when)(begin)

    if meanwhile is not None:
        meanwhile()
    for side, buf in enumerate(bufs):
        for n in range(len(pieces)):
            for who in range(CORES):
                pltpu.make_async_copy(other.at[side, n], buf.at[:, lanes(n, who)], sems.at[side, n, who]).wait()
    col_buf, row_buf = bufs
    if ready is not None:
        ready.wait()

    def rows(m, c):
        here = pl.ds(pl.multiple_of(m * ROW_TILE, ROW_TILE), ROW_TILE)
        left = row_buf[here, :]
        for start, size in COL_TILES:
            part = lax.dot_general(
                left, col_buf[start : start + size, :], (((1,), (1,)), ((), ())), preferred_element_type=jnp.float32
            )
            for at in range(0, size, LANES):
                wide = min(LANES, size - at)
                tile = acc.at[(start + at) // LANES, here, pl.ds(0, wide)]
                if fresh:
                    tile[...] = part[:, at : at + wide]
                else:
                    tile[...] += part[:, at : at + wide]
        return c

    lax.fori_loop(0, WIDTH // ROW_TILE, rows, 0)


def early_kernel(table, other, *rest, keys, job, fresh):
    before = None
    if not fresh:
        before, *rest = rest
    count = sum(map(len, keys))
    pieces = unflatten(rest[:count], keys)
    out, col_buf, row_buf, acc, sems, sem = rest[count:]

    @pl.when(table[MINE + 3 * job] == 1)
    def _():
        ready = None
        if not fresh:
            ready = pltpu.make_async_copy(before, acc, sem)
            ready.start()
        late = [{} for _ in keys]
        multiply(table, job, pieces, other, late, (col_buf, row_buf), sems, acc, fresh, ready)
        copy = pltpu.make_async_copy(acc, out, sem)
        copy.start()
        copy.wait()


def density_kernel(rdm, out, wide, lifted):
    out[...] = jnp.zeros(out.shape, out.dtype)
    lifted[...] = jnp.zeros(lifted.shape, jnp.float32)
    wide[...] = rdm[...].astype(jnp.float32)
    for v in range(NACT):
        lifted[:, v * TPAD : v * TPAD + NACT] = wide[:, v * NACT : (v + 1) * NACT]
    for t in range(NACT):
        out[t * TPAD : t * TPAD + NACT, :] = lifted[t * NACT : (t + 1) * NACT, :].astype(jnp.bfloat16)


def spread_density(rdm):
    order = NACT * NACT
    return pl.pallas_call(
        density_kernel,
        out_shape=jax.ShapeDtypeStruct((PACKED, PACKED), jnp.bfloat16),
        scratch_shapes=[pltpu.VMEM((order, order), jnp.float32), pltpu.VMEM((order, PACKED), jnp.float32)],
        name="density",
    )(rdm)


def finish_kernel(table, other, before, density, *rest, keys, late_keys, job):
    count = sum(map(len, keys))
    pieces = unflatten(rest[:count], keys)
    rest = rest[count:]
    count = sum(map(len, late_keys))
    late = unflatten(rest[:count], late_keys)
    out, col_buf, row_buf, acc, prior, spread, sems, sem = rest[count:]

    @pl.when(table[MINE + 3 * job] == 0)
    def _():
        out[...] = jnp.zeros(out.shape, out.dtype)

    @pl.when(table[MINE + 3 * job] == 1)
    def _():
        copy = pltpu.make_async_copy(before, prior.at[:, pl.ds(0, WIDTH), :], sem)

        def while_fetching():
            copy.start()
            for sums in (acc, prior):
                sums[:, WIDTH:, :] = jnp.zeros((TILES, sums.shape[1] - WIDTH, LANES), jnp.float32)

        multiply(table, job, pieces, other, late, (col_buf, row_buf), sems, acc, True, None, while_fetching)
        copy.wait()

        def group(g, carry):
            for i in range(GROUP):
                here = pl.ds(g * GROUP + i, TPAD, stride=VBLK)
                rows = [acc[c, here, :] + prior[c, here, :] for c in range(TILES)]
                rows = jnp.concatenate(rows, axis=1).astype(jnp.bfloat16)
                for t in range(NACT):
                    spread[t * TPAD : (t + 1) * TPAD, i * VBLK : (i + 1) * VBLK] = rows[:, t * VBLK : (t + 1) * VBLK]
            x = spread[...]
            y = jnp.dot(density[...], x, preferred_element_type=jnp.float32)
            out[pl.ds(g, 1), :] = jnp.sum(y * x.astype(jnp.float32), axis=0, keepdims=True)
            return carry

        lax.fori_loop(0, VBLK // GROUP, group, 0)


def product_scratch(sources, rows):
    depth = len(sources) * CORES * LANES
    return [
        pltpu.VMEM((WIDTH, depth), jnp.bfloat16),
        pltpu.VMEM((WIDTH, depth), jnp.bfloat16),
        pltpu.VMEM((TILES, rows, LANES), jnp.float32),
    ]


ROOM = pltpu.CompilerParams(vmem_limit_bytes=48 * 1024 * 1024)


def early(table, other, before, pieces, sources, job):
    keys = keys_of(pieces, sources)
    flat = flatten(pieces, keys, sources)
    fresh = before is None
    held = [] if fresh else [before]
    in_hbm = pl.BlockSpec(memory_space=HBM)
    return pl.pallas_call(
        lambda *refs: early_kernel(*refs, keys=keys, job=job, fresh=fresh),
        in_specs=[pl.BlockSpec(memory_space=pltpu.SMEM)] + [in_hbm] * (1 + len(held) + len(flat)),
        out_specs=in_hbm,
        out_shape=jax.ShapeDtypeStruct((TILES, WIDTH, LANES), jnp.float32),
        scratch_shapes=product_scratch(sources, WIDTH)
        + [pltpu.SemaphoreType.DMA((2, len(sources), CORES)), pltpu.SemaphoreType.DMA],
        compiler_params=ROOM,
        name="early",
    )(table, other, *held, *flat)


def finish(table, other, before, density, pieces, late, sources, job):
    keys = keys_of(pieces, sources)
    late_keys = keys_of(late, sources)
    flat = flatten(pieces, keys, sources) + flatten(late, late_keys, sources)
    in_hbm = pl.BlockSpec(memory_space=HBM)
    return pl.pallas_call(
        lambda *refs: finish_kernel(*refs, keys=keys, late_keys=late_keys, job=job),
        in_specs=[pl.BlockSpec(memory_space=pltpu.SMEM), in_hbm, in_hbm, pl.BlockSpec(memory_space=pltpu.VMEM)]
        + [in_hbm] * len(flat),
        out_specs=pl.BlockSpec(memory_space=pltpu.VMEM),
        out_shape=jax.ShapeDtypeStruct((VBLK // GROUP, GROUP * VBLK), jnp.float32),
        scratch_shapes=product_scratch(sources, VBLK * TPAD)
        + [
            pltpu.VMEM((TILES, VBLK * TPAD, LANES), jnp.float32),
            pltpu.VMEM((PACKED, GROUP * VBLK), jnp.bfloat16),
            pltpu.SemaphoreType.DMA((2, len(sources), CORES)),
            pltpu.SemaphoreType.DMA,
        ],
        compiler_params=ROOM,
        name="finish",
    )(table, other, before, density, *flat)


def ring_shift(hops):
    n = lax.axis_size("aux")
    return [(i, (i + hops * CORES) % n) for i in range(n)]


def to_other_core(x):
    n = lax.axis_size("aux")
    return lax.ppermute(x, "aux", [(i, i ^ 1) for i in range(n)])


def energies_of(paired, orbital_energy, pair_blocks):
    table = orbital_energy.reshape(NBLK, VBLK)
    rows = table[pair_blocks[:, 0]]
    cols = table[pair_blocks[:, 1]]
    energy = -paired / (rows[:, :, None] + cols[:, None, :])
    weight = jnp.where(pair_blocks[:, 0] == pair_blocks[:, 1], jnp.float32(1.0), jnp.float32(2.0))
    total = jnp.sum(weight * jnp.sum(energy, axis=(1, 2)))
    mine = lax.dynamic_index_in_dim(energy, lax.axis_index("aux"), 0, keepdims=False)
    mean_energy = total / (VBLK * VBLK * lax.axis_size("aux"))
    return mine, mean_energy.reshape(1)


def sources_within(low, high):
    return [s for s in range(-CHIPS // 2, CHIPS // 2) if low <= abs(s) <= high]


NEAREST = sources_within(0, 3)
NEAR = sources_within(4, 5)
FAR = sources_within(6, CHIPS)


LAST_SELECTED = 8


def both_cores(x):
    core = lax.axis_index("aux") % CORES
    other = to_other_core(x)
    return jnp.where(core == 0, jnp.stack([x, other]), jnp.stack([other, x]))


def of_everyone(x):
    n = lax.axis_size("aux")
    rings = [list(range(core, n, CORES)) for core in range(CORES)]
    chips = lax.all_gather(both_cores(x), "aux", axis_index_groups=rings)
    return chips.reshape(n, VBLK, VBLK)


def planned(table, me, slabs, rdm, orbital_energy, pair_blocks):
    sent = pack(me, table, slabs)
    pieces = {s: {} for s in range(-CHIPS // 2, CHIPS // 2)}
    late = {s: {} for s in range(-CHIPS // 2, CHIPS // 2)}

    def keep(source, offset, value, hop):
        source = (source + CHIPS // 2) % CHIPS - CHIPS // 2
        if -ABOVE <= offset <= BELOW:
            pieces[source][offset] = value
            if hop > LAST_SELECTED:
                late[source][offset] = to_other_core(value)

    right = {reach: sent[reach - 1] for reach in range(1, LONGEST + 1)}
    left = {reach: sent[LONGEST + reach - 1] for reach in range(1, LONGEST + 1)}
    for offset in OFFSETS:
        keep(0, offset, right[offset + ABOVE] if offset > -ABOVE else left[BELOW + ABOVE], 0)
    none_late = {s: {} for s in pieces}

    def exchange(pieces, sources, job):
        chosen = select(table, pieces, sources, job)
        return to_other_core(chosen)

    for hop in range(1, LONGEST + 1):
        for reach in range(LONGEST, hop - 1, -1):
            right[reach] = lax.ppermute(right[reach], "aux", ring_shift(1))
            left[reach] = lax.ppermute(left[reach], "aux", ring_shift(-1))
            keep(-hop, reach - ABOVE - hop, right[reach], hop)
            keep(hop, BELOW - reach + hop, left[reach], hop)
        if hop == 1:
            density = spread_density(rdm)
        if hop == 3:
            other = exchange(pieces, NEAREST, 0)
            sums = early(table, other, None, pieces, NEAREST, 0)
        if hop == 5:
            other = exchange(pieces, NEAR, 0)
            sums = early(table, other, sums, pieces, NEAR, 0)
        if hop == LAST_SELECTED:
            other = exchange(pieces, FAR, 0)
    paired = finish(table, other, sums, density, pieces, late, FAR, 0)

    def from_everyone(everyone, places):
        return energies_of(everyone[places].transpose(0, 2, 1), orbital_energy, pair_blocks)

    places = lax.dynamic_slice_in_dim(table, 24, pair_blocks.shape[0])
    everyone = of_everyone(paired)

    def with_second_job():
        other = exchange(pieces, NEAREST, 1)
        sums = early(table, other, None, pieces, NEAREST, 1)
        other = exchange(pieces, NEAR, 1)
        sums = early(table, other, sums, pieces, NEAR, 1)
        other = exchange(pieces, FAR, 1)
        extra = of_everyone(finish(table, other, sums, density, pieces, none_late, FAR, 1))
        return from_everyone(jnp.stack([everyone, extra], axis=1).reshape(-1, VBLK, VBLK), places)

    return lax.switch(
        jnp.where(table[0] == 1, 1 + table[17], 0),
        (
            lambda: unplanned(rdm, slabs, orbital_energy, pair_blocks),
            lambda: from_everyone(everyone, places // JOBS),
            with_second_job,
        ),
    )


def unplanned(rdm, slabs, orbital_energy, pair_blocks):
    local_rows = slabs.shape[0]
    blocked = slabs.reshape(local_rows, NBLK, WIDTH)
    sides = []
    for side in range(2):
        outgoing = jnp.take(blocked, pair_blocks[:, side], axis=1)
        arrived = lax.all_to_all(outgoing, "aux", split_axis=1, concat_axis=0, tiled=True)
        sides.append(arrived.reshape(-1, WIDTH))
    products = lax.dot_general(sides[0], sides[1], (((0,), (0,)), ((), ())), preferred_element_type=jnp.float32)
    reordered = (
        products.astype(jnp.bfloat16)
        .reshape(VBLK, NACT, VBLK, NACT)
        .transpose(0, 2, 1, 3)
        .reshape(VBLK * VBLK, NACT * NACT)
    )
    contracted = jnp.dot(reordered, rdm, preferred_element_type=jnp.float32)
    paired = jnp.sum(contracted * reordered.astype(jnp.float32), axis=1).reshape(VBLK, VBLK)
    return energies_of(lax.all_gather(paired, "aux"), orbital_energy, pair_blocks)


def per_device(slabs, rdm, orbital_energy, pair_blocks):
    me = lax.axis_index("aux").reshape(1).astype(jnp.int32)
    table = make_plan(me, pair_blocks)
    return planned(table, me, slabs, rdm, orbital_energy, pair_blocks)


def solution(mesh):
    return jax.shard_map(
        per_device,
        mesh=mesh,
        in_specs=(P(("groups", "aux"), None), P("groups", None), P("groups"), P("groups", None)),
        out_specs=(P(("groups", "aux"), None), P("groups")),
        check_vma=False,
    )
```
